32 devices in a mesh: rep: 2 (over y), ada: 4 (over z), tp: 4 (over x, core).
Axes of the slice: x: 2, y: 2, z: 4, core: 2. Of those that a mesh axis runs over, the one named last changes fastest.
Arguments:
- hidden: bfloat16 [256, 8192], P(('rep', 'ada')), parts along dimension 0, may hold values from -6 to 6
- input_norm_gain: bfloat16 [8192], replicated, may hold values from 0.5 to 1.5
- request_adapter: int32 [256], P(('rep', 'ada')), parts along dimension 0, may hold values from 0 to 15, as said below
- cache_fill_length: int32 [256], P(('rep', 'ada')), parts along dimension 0, may hold values from 1 to 512, as said below
- query_weight: bfloat16 [8192, 8192], P('ada', 'tp'), may hold values from -0.0625 to 0.0625
- key_weight: bfloat16 [8192, 1024], P('ada', 'tp'), may hold values from -0.0625 to 0.0625
- value_weight: bfloat16 [8192, 1024], P('ada', 'tp'), may hold values from -0.0625 to 0.0625
- output_weight: bfloat16 [8192, 8192], P('tp', 'ada'), may hold values from -0.0625 to 0.0625
- down_weight_all: bfloat16 [8192, 512], P('tp', 'ada'), may hold values from -0.0625 to 0.0625
- query_up_weight: bfloat16 [256, 8192], P('ada', 'tp'), may hold values from -1.5 to 1.5
- value_up_weight: bfloat16 [256, 1024], P('ada', 'tp'), may hold values from -1.5 to 1.5
- rotated_key_cache: bfloat16 [256, 512, 1024], P(('rep', 'ada'), None, 'tp'), parts along dimension 0, may hold values from -768 to 768
- stored_value_cache: bfloat16 [256, 512, 1024], P(('rep', 'ada'), None, 'tp'), parts along dimension 0, may hold values from -6 to 6
Outputs:
- layer_out: bfloat16 [256, 8192], P(('rep', 'tp'), 'ada'), parts along dimension 0
- new_key: bfloat16 [256, 1024], P(('rep', 'ada'), 'tp'), parts along dimension 0
- new_value: bfloat16 [256, 1024], P(('rep', 'ada'), 'tp'), parts along dimension 0
The draws below stay inside these ranges and needn't reach their ends.
There are 2 independent parts, one for each index of `rep`. The reference program is written for one: setup_inputs(seed, part) draws one part's arguments, and reference() takes and returns one part's arrays. A program takes and returns all parts, laid end to end along the dimension named above; an argument that names none is the same for every part. Nothing has to cross between parts.
Inputs may be any that keep to these rules, and one draw needn't show every extreme that they name: `request_adapter`: among the 32 requests of one ada index (aligned blocks), at most 16 name adapters of one group 4 * o to 4 * o + 3; in every draw one group is named by exactly 16 requests of every block. `cache_fill_length`: within each part of rep the 128 lengths sum to 32768, and some request of each part has exactly 512.
All inputs are finite; a program needn't handle non-finite values.
Results may differ from the reference program's by a relative error of at most 0.012.
The reference program's roundings to bfloat16 on the way count: a program that leaves them out, or rounds other values in their place, can miss the bound.
Values may be sent and summed in bfloat16 or wider, within the bound.
No kernel may reach another device: no remote copies, remote signals or barrier semaphores. Data moves between devices by JAX's collectives and lax.ppermute only.
A program may use at most 64 MiB of HBM per device.

```python
import jax
import jax.numpy as jnp
from jax import lax

MODEL_WIDTH = 8192
QUERY_HEAD_COUNT = 64
KEY_VALUE_HEADS = 8
HEAD_WIDTH = 128
ADAPTER_RANK = 16
ADP_DEV = 4
REQ_DEV = 32
CTX = 512
ADAPTER_COUNT = 16
REQUESTS = 128
CAP = 16


def block_owners(block_key, owner_rank, blocks_count):
    pool_owner = jnp.repeat(jnp.arange(blocks_count, dtype=jnp.int32), CAP)
    pool_size = blocks_count * CAP
    noise_term = jax.random.randint(jax.random.fold_in(block_key, 1), (pool_size,), 0, 4096)
    rank_of = owner_rank[pool_owner]
    score_value = noise_term + jnp.where(rank_of < 4, 4096, 0) + jnp.where(rank_of == 0, 8192, 0)
    distinct = score_value * pool_size + jnp.arange(pool_size, dtype=jnp.int32)
    ranking = jnp.argsort(-distinct)
    picked = pool_owner[ranking[:REQ_DEV]]
    shuffle = jax.random.permutation(jax.random.fold_in(block_key, 2), REQ_DEV)
    return picked[shuffle]


def draw_request_adapter(key, part):
    blocks_count = REQUESTS // REQ_DEV
    order_owners = jax.random.permutation(jax.random.fold_in(key, 11), blocks_count)
    owner_rank = jnp.argsort(order_owners).astype(jnp.int32)
    block_keys = jax.random.split(jax.random.fold_in(key, 12), blocks_count)
    owners = jax.vmap(lambda block_key: block_owners(block_key, owner_rank, blocks_count))(block_keys)
    sub_index = jax.random.randint(jax.random.fold_in(key, 13), (blocks_count, REQ_DEV), 0, ADP_DEV)
    return (owners * ADP_DEV + sub_index).reshape(REQUESTS).astype(jnp.int32)


def draw_cache_fill_length(key, part):
    others = REQUESTS - 1
    remaining = REQUESTS * CTX // 2 - CTX
    base_len = remaining // others
    extra_count = remaining - others * base_len
    lengths_rest = base_len + (jnp.arange(others, dtype=jnp.int32) < extra_count).astype(jnp.int32)
    reach = min(base_len - 1, CTX - base_len - 2)
    half_count = others // 2
    shifts = jax.random.randint(jax.random.fold_in(key, 31), (half_count,), -reach, reach + 1).astype(jnp.int32)
    lengths_rest = lengths_rest.at[:half_count].add(shifts)
    lengths_rest = lengths_rest.at[half_count:2 * half_count].add(-shifts)
    lengths_rest = lengths_rest[jax.random.permutation(jax.random.fold_in(key, 32), others)]
    complete = jnp.concatenate([jnp.full((1,), CTX, jnp.int32), lengths_rest.astype(jnp.int32)])
    return complete[jax.random.permutation(jax.random.fold_in(key, 33), REQUESTS)].astype(jnp.int32)


def draw_rotated_key_cache(key, part):
    drawn = jax.random.normal(jax.random.fold_in(key, 21), (REQUESTS, CTX, KEY_VALUE_HEADS * HEAD_WIDTH), jnp.float32)
    drawn = jnp.clip(drawn, -6.0, 6.0)
    return drawn.astype(jnp.bfloat16)


def block_scale(own_key, dims, shards, least, largest):
    def one(dim, blocks):
        steps = jax.random.uniform(jax.random.fold_in(jax.random.fold_in(own_key, 6), dim), (blocks,), jnp.float32, least / len(shards), largest / len(shards))
        return jnp.repeat(jnp.exp(steps), dims[dim] // blocks).reshape((-1,) + (1,) * (len(dims) - dim - 1))

    factor_of = one(*shards[0])
    for cut in shards[1:]:
        factor_of = factor_of * one(*cut)
    return factor_of


def gaussian(own_key, extent, spread, bound, cuts=(), kind=jnp.bfloat16):
    result = jax.random.normal(own_key, extent, jnp.float32) * spread
    if len(cuts) > 0:
        result = block_scale(own_key, extent, cuts, -0.22, 0.18) * result
    return jnp.clip(result, min=-bound, max=bound).astype(kind)


def setup_inputs(seed: int = 0, part: int = 0) -> dict:
    key_list = jax.random.split(jax.random.key(seed), 14)
    part_keys = jax.random.split(jax.random.fold_in(key_list[13], part), 14)
    hidden = gaussian(part_keys[0], (REQUESTS, MODEL_WIDTH), 1.0, 6.0, ((0, 4),))
    input_norm_gain = jnp.clip(1.0 + 0.1 * jax.random.normal(key_list[1], (MODEL_WIDTH,), jnp.float32), 0.5, 1.5).astype(jnp.bfloat16)
    request_adapter = draw_request_adapter(jax.random.fold_in(jax.random.fold_in(key_list[13], part), 71), part)
    cache_fill_length = draw_cache_fill_length(jax.random.fold_in(jax.random.fold_in(key_list[13], part), 71), part)
    query_weight = gaussian(key_list[4], (MODEL_WIDTH, QUERY_HEAD_COUNT * HEAD_WIDTH), MODEL_WIDTH ** -0.5, 0.0625, ((0, 4), (1, 4)))
    key_weight = gaussian(key_list[5], (MODEL_WIDTH, KEY_VALUE_HEADS * HEAD_WIDTH), MODEL_WIDTH ** -0.5, 0.0625, ((0, 4), (1, 4)))
    value_weight = gaussian(key_list[6], (MODEL_WIDTH, KEY_VALUE_HEADS * HEAD_WIDTH), MODEL_WIDTH ** -0.5, 0.0625, ((0, 4), (1, 4)))
    output_weight = gaussian(key_list[7], (QUERY_HEAD_COUNT * HEAD_WIDTH, MODEL_WIDTH), (QUERY_HEAD_COUNT * HEAD_WIDTH) ** -0.5, 0.0625, ((0, 4), (1, 4)))
    down_weight_all = gaussian(key_list[8], (MODEL_WIDTH, ADAPTER_COUNT * 2 * ADAPTER_RANK), MODEL_WIDTH ** -0.5, 0.0625, ((0, 4), (1, 4)))
    query_up_weight = gaussian(key_list[9], (ADAPTER_COUNT * ADAPTER_RANK, QUERY_HEAD_COUNT * HEAD_WIDTH), ADAPTER_RANK ** -0.5, 1.5, ((0, 4), (1, 4)))
    value_up_weight = gaussian(key_list[10], (ADAPTER_COUNT * ADAPTER_RANK, KEY_VALUE_HEADS * HEAD_WIDTH), ADAPTER_RANK ** -0.5, 1.5, ((0, 4), (1, 4)))
    rotated_key_cache = draw_rotated_key_cache(jax.random.fold_in(jax.random.fold_in(key_list[13], part), 71), part)
    stored_value_cache = gaussian(part_keys[12], (REQUESTS, CTX, KEY_VALUE_HEADS * HEAD_WIDTH), 1.0, 6.0, ((0, 4), (2, 4)))
    return {"hidden": hidden, "input_norm_gain": input_norm_gain, "request_adapter": request_adapter, "cache_fill_length": cache_fill_length, "query_weight": query_weight, "key_weight": key_weight, "value_weight": value_weight, "output_weight": output_weight, "down_weight_all": down_weight_all, "query_up_weight": query_up_weight, "value_up_weight": value_up_weight, "rotated_key_cache": rotated_key_cache, "stored_value_cache": stored_value_cache}


ADAPTER_SCALE = 2.0
EPSILON = 1e-05
ROPE_BASE = 500000.0

def rotary(vectors, positions):
    count_rows = vectors.shape[0]
    split_heads = vectors.reshape(count_rows, -1, HEAD_WIDTH)
    halfway = HEAD_WIDTH // 2
    frequency = ROPE_BASE ** (-2.0 * jnp.arange(halfway, dtype=jnp.float32) / HEAD_WIDTH)
    angles = positions.astype(jnp.float32)[:, None] * frequency[None, :]
    cosine = jnp.cos(angles)[:, None, :]
    sine_part = jnp.sin(angles)[:, None, :]
    leading = split_heads[..., :halfway]
    trailing = split_heads[..., halfway:]
    turned = jnp.concatenate([leading * cosine - trailing * sine_part, trailing * cosine + leading * sine_part], axis=-1)
    return turned.reshape(count_rows, -1)

def attend_one(operands):
    query_row, key_fresh, value_fresh, cached_keys, cached_values, length = operands
    groups = QUERY_HEAD_COUNT // KEY_VALUE_HEADS
    score_scale = HEAD_WIDTH ** (-0.5)
    query_heads = query_row.astype(jnp.float32).reshape(KEY_VALUE_HEADS, groups, HEAD_WIDTH)
    key_heads = cached_keys.astype(jnp.float32).reshape(CTX, KEY_VALUE_HEADS, HEAD_WIDTH)
    value_heads = cached_values.astype(jnp.float32).reshape(CTX, KEY_VALUE_HEADS, HEAD_WIDTH)
    scores = jnp.einsum('kgd,ckd->kgc', query_heads, key_heads) * score_scale
    own_score = jnp.einsum('kgd,kd->kg', query_heads, key_fresh.astype(jnp.float32).reshape(KEY_VALUE_HEADS, HEAD_WIDTH)) * score_scale
    in_cache = jnp.arange(CTX, dtype=jnp.int32) < length
    masked = jnp.where(in_cache[None, None, :], scores, -1e+30)
    row_max = jnp.maximum(lax.optimization_barrier(jnp.max(masked, axis=-1)), own_score)
    exp_terms = jnp.where(in_cache[None, None, :], jnp.exp(masked - row_max[..., None]), 0.0)
    own_exp = jnp.exp(own_score - row_max)
    denominator = lax.optimization_barrier(jnp.sum(exp_terms, axis=-1)) + own_exp
    weights_low = (exp_terms / denominator[..., None]).astype(jnp.bfloat16)
    own_low = (own_exp / denominator).astype(jnp.bfloat16)
    mixed_heads = jnp.einsum('kgc,ckd->kgd', weights_low.astype(jnp.float32), value_heads)
    mixed_heads = mixed_heads + own_low.astype(jnp.float32)[..., None] * value_fresh.astype(jnp.float32).reshape(KEY_VALUE_HEADS, 1, HEAD_WIDTH)
    return mixed_heads.reshape(-1).astype(jnp.bfloat16)

def reference(hidden, input_norm_gain, request_adapter, cache_fill_length, query_weight, key_weight, value_weight, output_weight, down_weight_all, query_up_weight, value_up_weight, rotated_key_cache, stored_value_cache):
    widened = hidden.astype(jnp.float32)
    inverse = lax.rsqrt(lax.optimization_barrier(jnp.mean(widened * widened, axis=-1, keepdims=True)) + EPSILON)
    normalized_input = (widened * inverse * input_norm_gain.astype(jnp.float32)[None, :]).astype(jnp.bfloat16)
    query_matrix_rows = jnp.dot(normalized_input, query_weight, preferred_element_type=jnp.float32)
    key_rows = jnp.dot(normalized_input, key_weight, preferred_element_type=jnp.float32)
    value_matrix_rows = jnp.dot(normalized_input, value_weight, preferred_element_type=jnp.float32)
    down_projected = jnp.dot(normalized_input, down_weight_all, preferred_element_type=jnp.float32)
    column_owner = jnp.arange(down_projected.shape[1], dtype=jnp.int32) // (2 * ADAPTER_RANK)
    chosen = jnp.where(column_owner[None, :] == request_adapter[:, None], down_projected, 0.0).astype(jnp.bfloat16)
    split_rank = chosen.reshape(REQUESTS, ADAPTER_COUNT, 2 * ADAPTER_RANK)
    query_down_part = split_rank[:, :, :ADAPTER_RANK].reshape(REQUESTS, ADAPTER_COUNT * ADAPTER_RANK)
    value_down_part = split_rank[:, :, ADAPTER_RANK:].reshape(REQUESTS, ADAPTER_COUNT * ADAPTER_RANK)
    query_matrix_rows = query_matrix_rows + ADAPTER_SCALE * jnp.dot(query_down_part, query_up_weight, preferred_element_type=jnp.float32)
    value_matrix_rows = value_matrix_rows + ADAPTER_SCALE * jnp.dot(value_down_part, value_up_weight, preferred_element_type=jnp.float32)
    rotated_query = rotary(query_matrix_rows, cache_fill_length).astype(jnp.bfloat16)
    new_key = rotary(key_rows, cache_fill_length).astype(jnp.bfloat16)
    new_value = value_matrix_rows.astype(jnp.bfloat16)
    context = lax.map(attend_one, (rotated_query, new_key, new_value, rotated_key_cache, stored_value_cache, cache_fill_length))
    projected = jnp.dot(context, output_weight, preferred_element_type=jnp.float32)
    layer_out = (widened + projected).astype(jnp.bfloat16)
    return (layer_out, new_key, new_value)
```

```python
import jax
import jax.numpy as jnp
from jax import lax
from jax.experimental import pallas as pl
from jax.experimental.pallas import tpu as pltpu
from jax.sharding import PartitionSpec as P

HEAD_WIDTH = 128
ADAPTER_RANK = 16


ADAPTER_SCALE = 2.0
EPSILON = 1e-05
ROPE_BASE = 500000.0


def attend_kernel(lengths, query, fresh_key, fresh_value, keys, values, out):
    batch = query.shape[0]
    slots = keys.shape[1]
    first = pl.program_id(0) * batch
    position = lax.broadcasted_iota(jnp.int32, (query.shape[1], slots), 1)
    scale = HEAD_WIDTH ** (-0.5)
    for j in range(batch):
        valid = position < lengths[first + j]
        q = query[j]
        scores = (
            lax.dot_general(
                q, keys[j], (((1,), (1,)), ((), ())), preferred_element_type=jnp.float32
            )
            * scale
        )
        own = (
            jnp.sum(
                q.astype(jnp.float32) * fresh_key[j].astype(jnp.float32), axis=1, keepdims=True
            )
            * scale
        )
        masked = jnp.where(valid, scores, -1e30)
        top = jnp.maximum(jnp.max(masked, axis=1, keepdims=True), own)
        terms = jnp.where(valid, jnp.exp(masked - top), 0.0)
        own_term = jnp.exp(own - top)
        total = jnp.sum(terms, axis=1, keepdims=True) + own_term
        weights = (terms / total).astype(jnp.bfloat16)
        own_weight = (own_term / total).astype(jnp.bfloat16).astype(jnp.float32)
        mixed = lax.dot_general(
            weights, values[j], (((1,), (0,)), ((), ())), preferred_element_type=jnp.float32
        )
        out[j] = (mixed + own_weight * fresh_value[j].astype(jnp.float32)).astype(jnp.bfloat16)


def attend(lengths, query, fresh_key, fresh_value, keys, values, head):
    rows, heads, width = query.shape
    slots = keys.shape[1]
    batch = 4
    return pl.pallas_call(
        attend_kernel,
        grid_spec=pltpu.PrefetchScalarGridSpec(
            num_scalar_prefetch=1,
            grid=(rows // batch,),
            in_specs=[
                pl.BlockSpec((batch, heads, width), lambda i, _: (i, 0, 0)),
                pl.BlockSpec((batch, 1, width), lambda i, _: (i, 0, 0)),
                pl.BlockSpec((batch, 1, width), lambda i, _: (i, 0, 0)),
                pl.BlockSpec((batch, slots, width), lambda i, _: (i, 0, head)),
                pl.BlockSpec((batch, slots, width), lambda i, _: (i, 0, head)),
            ],
            out_specs=pl.BlockSpec((batch, heads, width), lambda i, _: (i, 0, 0)),
        ),
        out_shape=jax.ShapeDtypeStruct((rows, heads, width), jnp.bfloat16),
        name="attend",
    )(lengths, query, fresh_key, fresh_value, keys, values)


def turn(vectors, cosine, sine):
    halfway = HEAD_WIDTH // 2
    leading = vectors[..., :halfway]
    trailing = vectors[..., halfway:]
    return jnp.concatenate(
        [leading * cosine - trailing * sine, trailing * cosine + leading * sine], axis=-1
    )


def shift(x, axis, step):
    count = lax.axis_size(axis)
    return lax.ppermute(x, axis, [(j, (j + step) % count) for j in range(count)])


def on_device(
    hidden,
    input_norm_gain,
    request_adapter,
    cache_fill_length,
    query_weight,
    key_weight,
    value_weight,
    output_weight,
    down_weight_all,
    query_up_weight,
    value_up_weight,
    rotated_key_cache,
    stored_value_cache,
):
    f32, bf16 = jnp.float32, jnp.bfloat16
    rows, model = hidden.shape
    owners = lax.axis_size("ada")
    parts = lax.axis_size("tp")
    me = lax.axis_index("ada")
    tp_index = lax.axis_index("tp")
    portion = down_weight_all.shape[0]
    block = model // owners
    grouped = down_weight_all.shape[1] // (2 * ADAPTER_RANK)
    capacity = max(2, (2 * rows + owners - 1) // owners)

    core = tp_index % 2
    half = block // 2
    arrived = []
    for s in range(1, owners):
        dest = (me + s) % owners
        piece = lax.dynamic_slice_in_dim(hidden, dest * block + core * half, half, 1)
        arrived.append(shift(piece, "ada", s))
    mine = jnp.concatenate(arrived, axis=0)
    other = lax.ppermute(mine, "tp", [(j, j ^ 1) for j in range(parts)])
    flip = core == 1
    raw = jnp.concatenate(
        [jnp.where(flip, other, mine), jnp.where(flip, mine, other)], axis=1
    )
    raw = jnp.concatenate(
        [lax.dynamic_slice_in_dim(hidden, me * block, block, 1), raw], axis=0
    )

    widened = hidden.astype(f32)
    inverse = lax.rsqrt(jnp.mean(widened * widened, axis=-1, keepdims=True) + EPSILON)
    gain = input_norm_gain.astype(f32)[None, :]

    high = lax.reduce_precision(inverse, 8, 7)
    middle = lax.reduce_precision(inverse - high, 8, 7)
    low = lax.reduce_precision(inverse - high - middle, 8, 7)
    owner_of = request_adapter // grouped
    sub_of = request_adapter % grouped
    row_ids = jnp.arange(rows, dtype=jnp.int32)
    same_owner = owner_of[:, None] == owner_of[None, :]
    earlier = row_ids[:, None] > row_ids[None, :]
    slot_of = jnp.sum(jnp.logical_and(same_owner, earlier), axis=1)
    my_slice = lax.dynamic_slice_in_dim(hidden, tp_index * portion, portion, 1).astype(f32)
    my_gain = lax.dynamic_slice_in_dim(input_norm_gain, tp_index * portion, portion, 0)
    my_normed = (my_slice * inverse * my_gain.astype(f32)[None, :]).astype(bf16)
    ids = jnp.stack([sub_of, row_ids], axis=1).astype(bf16)
    table = jnp.concatenate([my_normed, jnp.pad(ids, ((0, 0), (0, 126)))], axis=1)
    slots = jnp.arange(capacity, dtype=jnp.int32)
    pieces = jnp.concatenate([high, middle, low], axis=0).reshape(1, 3 * rows)
    pieces = jnp.pad(pieces, ((0, capacity - 1), (0, 128 - 3 * rows))).astype(bf16)
    routed = []
    for s in range(owners):
        dest = (me + s) % owners
        pick = jnp.logical_and(owner_of[None, :] == dest, slot_of[None, :] == slots[:, None])
        picked = jnp.dot(pick.astype(bf16), table, preferred_element_type=f32).astype(bf16)
        picked = jnp.concatenate([picked, pieces], axis=1)
        routed.append(shift(picked, "ada", s) if s else picked)
    routed = jnp.stack(routed)
    scales = routed[:, 0, portion + 128 : portion + 128 + 3 * rows].astype(f32)
    scales = scales[:, :rows] + scales[:, rows : 2 * rows] + scales[:, 2 * rows :]
    scales = scales.reshape(owners * rows, 1)
    sub_in = routed[:, :, portion].astype(jnp.int32).reshape(-1)
    row_in = routed[:, :, portion + 1].astype(jnp.int32)
    row_in = (jnp.arange(owners, dtype=jnp.int32)[:, None] * rows + row_in).reshape(-1)

    down_part = jnp.dot(
        routed[:, :, :portion].reshape(owners * capacity, portion),
        down_weight_all,
        preferred_element_type=f32,
    )
    down = down_part
    for s in range(1, parts):
        down = down + shift(down_part, "tp", s)
    column = jnp.arange(down.shape[1], dtype=jnp.int32)
    chosen = jnp.where((column // (2 * ADAPTER_RANK))[None, :] == sub_in[:, None], down, 0.0)
    chosen = chosen.astype(bf16)
    put = (jnp.arange(owners * rows, dtype=jnp.int32)[:, None] == row_in[None, :]).astype(bf16)
    placed = jnp.dot(put, chosen, preferred_element_type=f32).astype(bf16)
    inside = column % (2 * ADAPTER_RANK)
    target = (column // (2 * ADAPTER_RANK)) * ADAPTER_RANK + inside % ADAPTER_RANK
    target = target + jnp.where(inside < ADAPTER_RANK, 0, grouped * ADAPTER_RANK)
    order = (target[:, None] == column[None, :]).astype(bf16)
    placed = (ADAPTER_SCALE * jnp.dot(placed, order, preferred_element_type=f32)).astype(bf16)
    placed_query = placed[:, : grouped * ADAPTER_RANK]
    placed_value = placed[:, grouped * ADAPTER_RANK :]

    block_gain = lax.dynamic_slice_in_dim(input_norm_gain, me * block, block, 0)
    normed = (raw.astype(f32) * scales * block_gain.astype(f32)[None, :]).astype(bf16)
    heads = key_weight.shape[1] // HEAD_WIDTH
    groups = query_weight.shape[1] // key_weight.shape[1]
    wide = groups * HEAD_WIDTH
    frequency = ROPE_BASE ** (
        -2.0 * jnp.arange(HEAD_WIDTH // 2, dtype=f32) / HEAD_WIDTH
    )
    angles = cache_fill_length.astype(f32)[:, None] * frequency[None, :]
    cosine = jnp.cos(angles)[:, None, :]
    sine = jnp.sin(angles)[:, None, :]
    new_keys, new_values, outs = [], [], None
    for h in range(heads):
        qs = slice(h * wide, (h + 1) * wide)
        ks = slice(h * HEAD_WIDTH, (h + 1) * HEAD_WIDTH)
        query_part = jnp.dot(normed, query_weight[:, qs], preferred_element_type=f32)
        query_part = query_part + jnp.dot(
            placed_query, query_up_weight[:, qs], preferred_element_type=f32
        )
        key_part = jnp.dot(normed, key_weight[:, ks], preferred_element_type=f32)
        value_part = jnp.dot(normed, value_weight[:, ks], preferred_element_type=f32)
        value_part = value_part + jnp.dot(
            placed_value, value_up_weight[:, ks], preferred_element_type=f32
        )
        part = jnp.concatenate([query_part, key_part, value_part], axis=1)
        part = part.reshape(owners, rows, wide + 2 * HEAD_WIDTH)
        total = part[0]
        for s in range(1, owners):
            total = total + shift(part[s].astype(bf16), "ada", -s).astype(f32)
        total = total.reshape(rows, groups + 2, HEAD_WIDTH)
        turned = turn(total[:, : groups + 1], cosine, sine).astype(bf16)
        fresh_key = turned[:, groups:]
        fresh_value = total[:, groups + 1 :].astype(bf16)
        context = attend(
            cache_fill_length,
            turned[:, :groups],
            fresh_key,
            fresh_value,
            rotated_key_cache,
            stored_value_cache,
            h,
        ).reshape(rows, wide)
        gathered = [context] + [shift(context, "ada", s) for s in range(1, owners)]
        gathered = jnp.concatenate(gathered, axis=0)
        out = jnp.dot(gathered, output_weight[qs, :], preferred_element_type=f32)
        outs = out if outs is None else outs + out
        new_keys.append(fresh_key)
        new_values.append(fresh_value)
    new_key = jnp.concatenate(new_keys, axis=1).reshape(rows, -1)
    new_value = jnp.concatenate(new_values, axis=1).reshape(rows, -1)

    outs = outs.reshape(owners, rows, -1)
    raw = raw.reshape(owners, rows, block)
    per_part = owners // parts

    def blocks_of(stacked, part_index):
        found = [
            lax.dynamic_index_in_dim(
                stacked, (me - part_index * per_part - j) % owners, 0, keepdims=False
            )
            for j in range(per_part)
        ]
        return jnp.concatenate(found, axis=0)

    summed = blocks_of(raw, tp_index).astype(f32) + blocks_of(outs, tp_index)
    for s in range(1, parts):
        sent = blocks_of(outs, (tp_index + s) % parts).astype(bf16)
        summed = summed + shift(sent, "tp", s).astype(f32)
    return (summed.astype(bf16), new_key, new_value)


def solution(mesh):
    return jax.shard_map(
        on_device,
        mesh=mesh,
        in_specs=(
            P(("rep", "ada"), None),
            P(),
            P(("rep", "ada")),
            P(("rep", "ada")),
            P("ada", "tp"),
            P("ada", "tp"),
            P("ada", "tp"),
            P("tp", "ada"),
            P("tp", "ada"),
            P("ada", "tp"),
            P("ada", "tp"),
            P(("rep", "ada"), None, "tp"),
            P(("rep", "ada"), None, "tp"),
        ),
        out_specs=(P(("rep", "tp"), "ada"), P(("rep", "ada"), "tp"), P(("rep", "ada"), "tp")),
        check_vma=False,
    )
```

```python
import jax
import jax.numpy as jnp
from jax import lax
from jax.experimental import pallas as pl
from jax.experimental.pallas import tpu as pltpu
from jax.sharding import PartitionSpec as P

HEAD_WIDTH = 128
ADAPTER_RANK = 16


ADAPTER_SCALE = 2.0
EPSILON = 1e-05
ROPE_BASE = 500000.0


def attend_kernel(lengths, query, fresh_key, fresh_value, keys, values, out):
    batch, heads, _ = query.shape
    slots = keys.shape[1]
    count = batch * heads
    first = pl.program_id(0) * batch
    scale = HEAD_WIDTH ** (-0.5)
    scores = jnp.concatenate(
        [
            lax.dot_general(
                query[j], keys[j], (((1,), (1,)), ((), ())), preferred_element_type=jnp.float32
            )
            for j in range(batch)
        ],
        axis=0,
    )
    limit = jnp.concatenate(
        [jnp.full((heads, slots), lengths[first + j], jnp.int32) for j in range(batch)], axis=0
    )
    valid = lax.broadcasted_iota(jnp.int32, (count, slots), 1) < limit
    own = jnp.concatenate(
        [
            jnp.sum(
                query[j].astype(jnp.float32) * fresh_key[j].astype(jnp.float32),
                axis=1,
                keepdims=True,
            )
            for j in range(batch)
        ],
        axis=0,
    )
    own = own * scale
    masked = jnp.where(valid, scores * scale, -1e30)
    top = jnp.maximum(jnp.max(masked, axis=1, keepdims=True), own)
    terms = jnp.where(valid, jnp.exp(masked - top), 0.0)
    own_term = jnp.exp(own - top)
    total = jnp.sum(terms, axis=1, keepdims=True) + own_term
    weights = terms / total
    own_weight = (own_term / total).astype(jnp.bfloat16).astype(jnp.float32)
    for j in range(batch):
        span = slice(j * heads, (j + 1) * heads)
        mixed = lax.dot_general(
            weights[span].astype(jnp.bfloat16),
            values[j],
            (((1,), (0,)), ((), ())),
            preferred_element_type=jnp.float32,
        )
        fresh = own_weight[span] * fresh_value[j].astype(jnp.float32)
        out[j] = (mixed + fresh).astype(jnp.bfloat16)


def attend(lengths, query, fresh_key, fresh_value, keys, values, head):
    rows, heads, width = query.shape
    slots = keys.shape[1]
    batch = 8
    return pl.pallas_call(
        attend_kernel,
        grid_spec=pltpu.PrefetchScalarGridSpec(
            num_scalar_prefetch=1,
            grid=(rows // batch,),
            in_specs=[
                pl.BlockSpec((batch, heads, width), lambda i, _: (i, 0, 0)),
                pl.BlockSpec((batch, 1, width), lambda i, _: (i, 0, 0)),
                pl.BlockSpec((batch, 1, width), lambda i, _: (i, 0, 0)),
                pl.BlockSpec((batch, slots, width), lambda i, _: (i, 0, head)),
                pl.BlockSpec((batch, slots, width), lambda i, _: (i, 0, head)),
            ],
            out_specs=pl.BlockSpec((batch, heads, width), lambda i, _: (i, 0, 0)),
        ),
        out_shape=jax.ShapeDtypeStruct((rows, heads, width), jnp.bfloat16),
        name="attend",
    )(lengths, query, fresh_key, fresh_value, keys, values)


def turn(vectors, cosine, sine):
    halfway = HEAD_WIDTH // 2
    leading = vectors[..., :halfway]
    trailing = vectors[..., halfway:]
    return jnp.concatenate(
        [leading * cosine - trailing * sine, trailing * cosine + leading * sine], axis=-1
    )


def shift(x, axis, step):
    count = lax.axis_size(axis)
    return lax.ppermute(x, axis, [(j, (j + step) % count) for j in range(count)])


def on_device(
    hidden,
    input_norm_gain,
    request_adapter,
    cache_fill_length,
    query_weight,
    key_weight,
    value_weight,
    output_weight,
    down_weight_all,
    query_up_weight,
    value_up_weight,
    rotated_key_cache,
    stored_value_cache,
):
    f32, bf16 = jnp.float32, jnp.bfloat16
    rows, model = hidden.shape
    owners = lax.axis_size("ada")
    parts = lax.axis_size("tp")
    me = lax.axis_index("ada")
    tp_index = lax.axis_index("tp")
    portion = down_weight_all.shape[0]
    block = model // owners
    grouped = down_weight_all.shape[1] // (2 * ADAPTER_RANK)
    capacity = max(2, (2 * rows + owners - 1) // owners)

    core = tp_index % 2
    half = block // 2
    arrived = []
    for s in range(1, owners):
        dest = (me + s) % owners
        piece = lax.dynamic_slice_in_dim(hidden, dest * block + core * half, half, 1)
        arrived.append(shift(piece, "ada", s))
    mine = jnp.concatenate(arrived, axis=0)
    other = lax.ppermute(mine, "tp", [(j, j ^ 1) for j in range(parts)])
    flip = core == 1
    raw = jnp.concatenate(
        [jnp.where(flip, other, mine), jnp.where(flip, mine, other)], axis=1
    )
    raw = jnp.concatenate(
        [lax.dynamic_slice_in_dim(hidden, me * block, block, 1), raw], axis=0
    )

    widened = hidden.astype(f32)
    inverse = lax.rsqrt(jnp.mean(widened * widened, axis=-1, keepdims=True) + EPSILON)
    gain = input_norm_gain.astype(f32)[None, :]

    high = lax.reduce_precision(inverse, 8, 7)
    middle = lax.reduce_precision(inverse - high, 8, 7)
    low = lax.reduce_precision(inverse - high - middle, 8, 7)
    owner_of = request_adapter // grouped
    sub_of = request_adapter % grouped
    row_ids = jnp.arange(rows, dtype=jnp.int32)
    same_owner = owner_of[:, None] == owner_of[None, :]
    earlier = row_ids[:, None] > row_ids[None, :]
    slot_of = jnp.sum(jnp.logical_and(same_owner, earlier), axis=1)
    my_slice = lax.dynamic_slice_in_dim(hidden, tp_index * portion, portion, 1).astype(f32)
    my_gain = lax.dynamic_slice_in_dim(input_norm_gain, tp_index * portion, portion, 0)
    my_normed = (my_slice * inverse * my_gain.astype(f32)[None, :]).astype(bf16)
    ids = jnp.stack([sub_of, row_ids], axis=1).astype(bf16)
    table = jnp.concatenate([my_normed, jnp.pad(ids, ((0, 0), (0, 126)))], axis=1)
    slots = jnp.arange(capacity, dtype=jnp.int32)
    pieces = jnp.concatenate([high, middle, low], axis=0).reshape(1, 3 * rows)
    pieces = jnp.pad(pieces, ((0, capacity - 1), (0, 128 - 3 * rows))).astype(bf16)
    routed = []
    for s in range(owners):
        dest = (me + s) % owners
        pick = jnp.logical_and(owner_of[None, :] == dest, slot_of[None, :] == slots[:, None])
        picked = jnp.dot(pick.astype(bf16), table, preferred_element_type=f32).astype(bf16)
        picked = jnp.concatenate([picked, pieces], axis=1)
        routed.append(shift(picked, "ada", s) if s else picked)
    routed = jnp.stack(routed)
    scales = routed[:, 0, portion + 128 : portion + 128 + 3 * rows].astype(f32)
    scales = scales[:, :rows] + scales[:, rows : 2 * rows] + scales[:, 2 * rows :]
    scales = scales.reshape(owners * rows, 1)
    sub_in = routed[:, :, portion].astype(jnp.int32).reshape(-1)
    row_in = routed[:, :, portion + 1].astype(jnp.int32)
    row_in = (jnp.arange(owners, dtype=jnp.int32)[:, None] * rows + row_in).reshape(-1)

    down_part = jnp.dot(
        routed[:, :, :portion].reshape(owners * capacity, portion),
        down_weight_all,
        preferred_element_type=f32,
    )
    down = down_part
    for s in range(1, parts):
        down = down + shift(down_part, "tp", s)
    column = jnp.arange(down.shape[1], dtype=jnp.int32)
    chosen = jnp.where((column // (2 * ADAPTER_RANK))[None, :] == sub_in[:, None], down, 0.0)
    chosen = chosen.astype(bf16)
    put = (jnp.arange(owners * rows, dtype=jnp.int32)[:, None] == row_in[None, :]).astype(bf16)
    placed = jnp.dot(put, chosen, preferred_element_type=f32).astype(bf16)
    inside = column % (2 * ADAPTER_RANK)
    target = (column // (2 * ADAPTER_RANK)) * ADAPTER_RANK + inside % ADAPTER_RANK
    target = target + jnp.where(inside < ADAPTER_RANK, 0, grouped * ADAPTER_RANK)
    order = (target[:, None] == column[None, :]).astype(bf16)
    placed = (ADAPTER_SCALE * jnp.dot(placed, order, preferred_element_type=f32)).astype(bf16)
    placed_query = placed[:, : grouped * ADAPTER_RANK]
    placed_value = placed[:, grouped * ADAPTER_RANK :]

    block_gain = lax.dynamic_slice_in_dim(input_norm_gain, me * block, block, 0)
    normed = (raw.astype(f32) * scales * block_gain.astype(f32)[None, :]).astype(bf16)
    heads = key_weight.shape[1] // HEAD_WIDTH
    groups = query_weight.shape[1] // key_weight.shape[1]
    wide = groups * HEAD_WIDTH
    frequency = ROPE_BASE ** (
        -2.0 * jnp.arange(HEAD_WIDTH // 2, dtype=f32) / HEAD_WIDTH
    )
    angles = cache_fill_length.astype(f32)[:, None] * frequency[None, :]
    cosine = jnp.cos(angles)[:, None, :]
    sine = jnp.sin(angles)[:, None, :]
    new_keys, new_values, outs = [], [], None
    for h in range(heads):
        qs = slice(h * wide, (h + 1) * wide)
        ks = slice(h * HEAD_WIDTH, (h + 1) * HEAD_WIDTH)
        query_part = jnp.dot(normed, query_weight[:, qs], preferred_element_type=f32)
        query_part = query_part + jnp.dot(
            placed_query, query_up_weight[:, qs], preferred_element_type=f32
        )
        key_part = jnp.dot(normed, key_weight[:, ks], preferred_element_type=f32)
        value_part = jnp.dot(normed, value_weight[:, ks], preferred_element_type=f32)
        value_part = value_part + jnp.dot(
            placed_value, value_up_weight[:, ks], preferred_element_type=f32
        )
        part = jnp.concatenate([query_part, key_part, value_part], axis=1)
        part = part.reshape(owners, rows, wide + 2 * HEAD_WIDTH)
        moved = [shift(part[s].astype(bf16), "ada", -s) for s in range(1, owners)]
        if h:
            moved, _ = lax.optimization_barrier((moved, context))
        total = part[0]
        for piece in moved:
            total = total + piece.astype(f32)
        total = total.reshape(rows, groups + 2, HEAD_WIDTH)
        turned = turn(total[:, : groups + 1], cosine, sine).astype(bf16)
        fresh_key = turned[:, groups:]
        fresh_value = total[:, groups + 1 :].astype(bf16)
        context = attend(
            cache_fill_length,
            turned[:, :groups],
            fresh_key,
            fresh_value,
            rotated_key_cache,
            stored_value_cache,
            h,
        )
        context = context.reshape(rows, wide)
        gathered = [context] + [shift(context, "ada", s) for s in range(1, owners)]
        gathered = jnp.concatenate(gathered, axis=0)
        out = jnp.dot(gathered, output_weight[qs, :], preferred_element_type=f32)
        outs = lax.optimization_barrier(out) if outs is None else outs + out
        new_keys.append(fresh_key)
        new_values.append(fresh_value)
    new_key = jnp.concatenate(new_keys, axis=1).reshape(rows, -1)
    new_value = jnp.concatenate(new_values, axis=1).reshape(rows, -1)

    outs = outs.reshape(owners, rows, -1)
    raw = raw.reshape(owners, rows, block)
    per_part = owners // parts

    def blocks_of(stacked, part_index):
        found = [
            lax.dynamic_index_in_dim(
                stacked, (me - part_index * per_part - j) % owners, 0, keepdims=False
            )
            for j in range(per_part)
        ]
        return jnp.concatenate(found, axis=0)

    summed = blocks_of(raw, tp_index).astype(f32) + blocks_of(outs, tp_index)
    for s in range(1, parts):
        sent = blocks_of(outs, (tp_index + s) % parts).astype(bf16)
        summed = summed + shift(sent, "tp", s).astype(f32)
    return (summed.astype(bf16), new_key, new_value)


def solution(mesh):
    return jax.shard_map(
        on_device,
        mesh=mesh,
        in_specs=(
            P(("rep", "ada"), None),
            P(),
            P(("rep", "ada")),
            P(("rep", "ada")),
            P("ada", "tp"),
            P("ada", "tp"),
            P("ada", "tp"),
            P("tp", "ada"),
            P("tp", "ada"),
            P("ada", "tp"),
            P("ada", "tp"),
            P(("rep", "ada"), None, "tp"),
            P(("rep", "ada"), None, "tp"),
        ),
        out_specs=(P(("rep", "tp"), "ada"), P(("rep", "ada"), "tp"), P(("rep", "ada"), "tp")),
        check_vma=False,
    )
```
